32 devices in a mesh: grp: 1, dev: 32 (over z, y, x, core).
Axes of the slice: x: 2, y: 2, z: 4, core: 2. Of those that a mesh axis runs over, the one named last changes fastest.
Arguments:
- points: float32 [32768, 768], P(('grp', 'dev')), may hold values from -12 to 12
- assignment: int32 [32768], P(('grp', 'dev')), may hold values from 0 to 8191, as said below
Outputs:
- centroids: float32 [8192, 768], P('dev')
- spread: float32 [8192], P('dev')
The draws below stay inside these ranges and needn't reach their ends.
Inputs may be any that keep to these rules, and one draw needn't show every extreme that they name: `assignment`: the owner of cluster c is c // 256. Among the 1024 points of one device (aligned blocks of 1024), at most 64 belong to clusters of one owner; some owner receives exactly 64 from every device's block.
All inputs are finite; a program needn't handle non-finite values.
Results may differ from the reference program's by a relative error of at most 0.000071.
Values sent between devices are 32-bit elements; how exact they have to be, the bound alone decides.
A program may use at most 64 MiB of HBM per device.

```python
import jax
import jax.numpy as jnp
from jax import lax

D = 768
CL_OWN = 256
TOK_DEV = 1024
CLUSTERS = 8192
CAP = 64
POINTS = 32768


def draw_assignment(key, part):
    blocks = POINTS // TOK_DEV
    owners = CLUSTERS // CL_OWN
    total_slots = owners * CAP
    key_hot, key_score, key_order, key_within = jax.random.split(key, 4)
    hottest = jax.random.randint(key_hot, (), 0, owners)
    scores = jax.random.randint(key_score, (blocks, total_slots), 0, 1 << 16)
    slot_owner = jnp.arange(total_slots, dtype=jnp.int32) // CAP
    scores = jnp.where(slot_owner[None, :] == hottest, scores + (1 << 17), scores)
    distinct = scores * total_slots + jnp.arange(total_slots, dtype=jnp.int32)[None, :]
    _, chosen = lax.top_k(distinct, TOK_DEV)
    shuffle = jax.random.randint(key_order, (blocks, TOK_DEV), 0, 1 << 18)
    shuffle = shuffle * TOK_DEV + jnp.arange(TOK_DEV, dtype=jnp.int32)[None, :]
    order = jnp.argsort(shuffle, axis=1)
    picked = jnp.take_along_axis(chosen.astype(jnp.int32), order, axis=1)
    owner = picked // CAP
    within = jax.random.randint(key_within, (blocks, TOK_DEV), 0, CL_OWN)
    return (owner * CL_OWN + within).reshape(-1).astype(jnp.int32)


def block_levels(stream_key, dims, shards, smallest, largest):
    gain, own = 1.0, jax.random.fold_in(stream_key, 6)
    for dim, parts in shards:
        steps = jnp.exp(jax.random.uniform(jax.random.fold_in(own, dim), (parts,), jnp.float32, smallest / len(shards), largest / len(shards)))
        gain = gain * jnp.repeat(steps, dims[dim] // parts).reshape([-1 if axis == dim else 1 for axis in range(len(dims))])
    return gain


def bell_draw(stream_key, extent, width, limit, shards=(), held_as=jnp.bfloat16):
    drawn = width * jax.random.normal(stream_key, extent, jnp.float32)
    if shards:
        drawn = drawn * block_levels(stream_key, extent, shards, -0.22, 0.18)
    return jnp.clip(drawn, -limit, limit).astype(held_as)


def setup_inputs(seed: int = 0) -> dict:
    key_of = jax.random.split(jax.random.key(seed), 3)
    points = bell_draw(key_of[0], (POINTS, D), 2.0, 12.0, ((0, 32),), jnp.float32)
    assignment = draw_assignment(jax.random.fold_in(key_of[2], 71), 0)
    return dict(points=points, assignment=assignment)


def reference(points, assignment):
    sums = jax.ops.segment_sum(points, assignment, num_segments=CLUSTERS)
    counts = jax.ops.segment_sum(jnp.ones(assignment.shape, jnp.float32), assignment, num_segments=CLUSTERS)
    squares = jax.ops.segment_sum(jnp.sum(points * points, axis=1), assignment, num_segments=CLUSTERS)
    denom = jnp.maximum(counts, 1.0)
    centroids = sums / denom[:, None]
    spread = (squares - jnp.sum(sums * sums, axis=1) / denom) / (denom * D)
    return centroids, spread
```

```python
import functools

import jax
import jax.numpy as jnp
from jax import lax
from jax.experimental import pallas as pl
from jax.experimental.pallas import tpu as pltpu
from jax.sharding import PartitionSpec as P

CL_OWN = 256
LANES = 128
MESH = pl.DeviceIdType.MESH


def finish(sums, counts, squares):
    denom = jnp.maximum(counts, 1.0)
    centre = sums / denom[:, None]
    spread = (squares - jnp.sum(sums * sums, axis=1) / denom) / (denom * sums.shape[1])
    return (centre, spread)


def pieces(value, count):
    out = []
    for _ in range(count):
        part = value.astype(jnp.bfloat16)
        out.append(part)
        value = value - part.astype(jnp.float32)
    return out


def kernel(
    inner, outer, cap, order,
    points_ref, target_ref, meta_ref, sums_ref, aux_ref,
    high, low, out, got, got_meta, zout, zgot, zaux, zgot_aux,
    meta_send, meta_recv, send, recv, zsend, zrecv, zaux_send, zaux_recv,
):
    me = lax.axis_index("dev")
    plane = me // inner
    seat = lax.rem(me, inner)
    rows = points_ref.shape[0]
    width = points_ref.shape[1]
    rep = LANES // cap

    barrier = pltpu.get_barrier_semaphore()
    for d in range(1, inner):
        peer = plane * inner + lax.rem(seat + d, inner)
        pl.semaphore_signal(barrier, inc=1, device_id={"dev": peer}, device_id_type=MESH)
    for d in range(1, outer):
        peer = lax.rem(plane + d, outer) * inner + seat
        pl.semaphore_signal(barrier, inc=1, device_id={"dev": peer}, device_id_type=MESH)
    pl.semaphore_wait(barrier, inner + outer - 2)

    def meta_copy(d, source):
        p = lax.rem(seat + d, inner)
        s = lax.rem(seat + inner - d, inner) if source else seat
        return pltpu.make_async_remote_copy(
            src_ref=meta_ref.at[p],
            dst_ref=got_meta.at[s],
            send_sem=meta_send.at[d],
            recv_sem=meta_recv.at[d],
            device_id={"dev": plane * inner + p},
            device_id_type=MESH,
        )

    def data_copy(j, d, source):
        p = lax.rem(seat + d, inner)
        s = lax.rem(seat + inner - d, inner) if source else seat
        return pltpu.make_async_remote_copy(
            src_ref=out.at[j, p],
            dst_ref=got.at[j, s],
            send_sem=send.at[j, d],
            recv_sem=recv.at[j, d],
            device_id={"dev": plane * inner + p},
            device_id_type=MESH,
        )

    def z_copies(j):
        device = {"dev": lax.rem(plane + order[j], outer) * inner + seat}
        return (
            pltpu.make_async_remote_copy(
                src_ref=zout.at[j], dst_ref=zgot.at[j], send_sem=zsend.at[j], recv_sem=zrecv.at[j],
                device_id=device, device_id_type=MESH,
            ),
            pltpu.make_async_remote_copy(
                src_ref=zaux.at[j], dst_ref=zgot_aux.at[j], send_sem=zaux_send.at[j],
                recv_sem=zaux_recv.at[j], device_id=device, device_id_type=MESH,
            ),
        )

    for d in range(1, inner):
        meta_copy(d, False).start()

    value = points_ref[...]
    top = value.astype(jnp.bfloat16)
    high[...] = top
    low[...] = (value - top.astype(jnp.float32)).astype(jnp.bfloat16)

    for j in range(outer):
        k = lax.rem(plane + order[j], outer)
        slot = k * (inner * cap) + lax.broadcasted_iota(jnp.int32, (inner * cap, rows), 0)
        pick = (slot == target_ref[...]).astype(jnp.bfloat16)
        block = jnp.dot(pick, high[...], preferred_element_type=jnp.float32)
        block = block + jnp.dot(pick, low[...], preferred_element_type=jnp.float32)
        out[j] = block.reshape(inner, cap, width)
        for d in range(1, inner):
            data_copy(j, d, False).start()

    for d in range(1, inner):
        meta_copy(d, True).wait_recv()
    got_meta[seat] = meta_ref[seat]

    cluster = lax.broadcasted_iota(jnp.int32, (CL_OWN, LANES), 0).astype(jnp.float32)
    lane = lax.broadcasted_iota(jnp.int32, (1, LANES), 1)
    first = (lane < cap).astype(jnp.float32)
    for j in range(outer):
        k = lax.rem(plane + order[j], outer)
        hits, weights = [], []
        for s in range(inner):
            tags = got_meta[s, k, 0:1, :]
            hits.append((cluster == tags).astype(jnp.bfloat16))
            norms = got_meta[s, k, 1:2, :]
            weights.append(
                jnp.concatenate(
                    [first.astype(jnp.bfloat16)] + pieces(norms, 3)
                    + [jnp.zeros((4, LANES), jnp.bfloat16)],
                    axis=0,
                )
            )
        hit = jnp.concatenate(hits, axis=1)
        weight = jnp.concatenate(weights, axis=1)
        aux = lax.dot_general(
            weight, hit, (((1,), (1,)), ((), ())), preferred_element_type=jnp.float32
        )
        for d in range(1, inner):
            data_copy(j, d, True).wait_recv()
        got[j, seat] = out[j, seat]
        stack = []
        for s in range(inner):
            stack.extend(pieces(got[j, s], rep))
        total = jnp.dot(hit, jnp.concatenate(stack, axis=0), preferred_element_type=jnp.float32)
        if j < outer - 1:
            zaux[j] = aux
            zout[j] = total
            for copy in z_copies(j):
                copy.start()
        else:
            sums_ref[...] = total
            aux_ref[...] = aux

    for j in range(outer - 1):
        for copy in z_copies(j):
            copy.wait_recv()
        sums_ref[...] += zgot[j]
        aux_ref[...] += zgot_aux[j]

    for d in range(1, inner):
        meta_copy(d, False).wait_send()
        for j in range(outer):
            data_copy(j, d, False).wait_send()
    for j in range(outer - 1):
        for copy in z_copies(j):
            copy.wait_send()


def body(points, assignment):
    owners = lax.axis_size("dev")
    rows, width = points.shape
    cap = 2 * rows // owners
    inner = 1
    while 4 * inner * inner <= 2 * owners:
        inner *= 2
    outer = owners // inner
    order = sorted(range(1, outer), key=lambda d: (-min(d, outer - d), d)) + [0]

    owner = assignment // CL_OWN
    local_label = assignment % CL_OWN
    matches = (owner[:, None] == jnp.arange(owners, dtype=jnp.int32)[None, :]).astype(jnp.float32)
    earlier = (jnp.arange(rows)[:, None] > jnp.arange(rows)[None, :]).astype(jnp.float32)
    before = jnp.dot(earlier, matches, preferred_element_type=jnp.float32)
    position = jnp.sum(before * matches, axis=1).astype(jnp.int32)
    target = owner * cap + position

    norms = jnp.sum(points * points, axis=1)
    held = target[None, :] == jnp.arange(owners * cap, dtype=jnp.int32)[:, None]
    tags = jnp.sum(jnp.where(held, local_label[None, :] + 1, 0), axis=1) - 1
    slot_norms = jnp.sum(jnp.where(held, norms[None, :], 0.0), axis=1)
    tags = tags.astype(jnp.float32).reshape(outer, inner, 1, cap)
    slot_norms = slot_norms.reshape(outer, inner, 1, cap)
    meta = jnp.concatenate(
        [
            jnp.tile(tags, (1, 1, 1, LANES // cap)),
            jnp.pad(slot_norms, ((0, 0), (0, 0), (0, 0), (0, LANES - cap))),
            jnp.zeros((outer, inner, 6, LANES), jnp.float32),
        ],
        axis=2,
    ).transpose(1, 0, 2, 3)

    f32, b16 = jnp.float32, jnp.bfloat16
    dma = pltpu.SemaphoreType.DMA
    hops = max(outer - 1, 1)
    sums, aux = pl.pallas_call(
        functools.partial(kernel, inner, outer, cap, order),
        out_shape=(
            jax.ShapeDtypeStruct((CL_OWN, width), f32),
            jax.ShapeDtypeStruct((8, CL_OWN), f32),
        ),
        in_specs=[pl.BlockSpec(memory_space=pltpu.VMEM)] * 3,
        out_specs=[pl.BlockSpec(memory_space=pltpu.VMEM)] * 2,
        scratch_shapes=[
            pltpu.VMEM((rows, width), b16),
            pltpu.VMEM((rows, width), b16),
            pltpu.VMEM((outer, inner, cap, width), f32),
            pltpu.VMEM((outer, inner, cap, width), f32),
            pltpu.VMEM((inner, outer, 8, LANES), f32),
            pltpu.VMEM((hops, CL_OWN, width), f32),
            pltpu.VMEM((hops, CL_OWN, width), f32),
            pltpu.VMEM((hops, 8, CL_OWN), f32),
            pltpu.VMEM((hops, 8, CL_OWN), f32),
            dma((inner,)), dma((inner,)),
            dma((outer, inner)), dma((outer, inner)),
            dma((hops,)), dma((hops,)), dma((hops,)), dma((hops,)),
        ],
        compiler_params=pltpu.CompilerParams(
            collective_id=0, has_side_effects=True, vmem_limit_bytes=60 * 1024 * 1024
        ),
    )(points, target[None, :], meta)
    counts = aux[0]
    squares = aux[1] + aux[2] + aux[3]
    sums, counts, squares = lax.psum((sums, counts, squares), "grp")
    return finish(sums, counts, squares)


def solution(mesh):
    return jax.shard_map(
        body,
        mesh=mesh,
        in_specs=(P(("grp", "dev"), None), P(("grp", "dev"))),
        out_specs=(P("dev", None), P("dev")),
        check_vma=False,
    )
```

```python
import functools

import jax
import jax.numpy as jnp
from jax import lax
from jax.experimental import pallas as pl
from jax.experimental.pallas import tpu as pltpu
from jax.sharding import PartitionSpec as P

CL_OWN = 256
LANES = 128
MESH = pl.DeviceIdType.MESH


def finish(sums, counts, squares):
    denom = jnp.maximum(counts, 1.0)
    centre = sums / denom[:, None]
    spread = (squares - jnp.sum(sums * sums, axis=1) / denom) / (denom * sums.shape[1])
    return (centre, spread)


def pieces(value, count):
    out = []
    for _ in range(count):
        part = value.astype(jnp.bfloat16)
        out.append(part)
        value = value - part.astype(jnp.float32)
    return out


def kernel(
    inner, outer, cap, chunk,
    points_ref, route_ref, sums_ref, aux_ref,
    high, low, facts, hit, out, got, mout, mgot, zout, zin, zaux, zin_aux,
    msend, mrecv, send, recv, zsend, zrecv, asend, arecv,
):
    me = lax.axis_index("dev")
    plane = me // inner
    seat = lax.rem(me, inner)
    rows, width = points_ref.shape
    chunks = width // chunk
    rep = LANES // cap
    last = outer - 1
    rights, lefts = last - plane, plane

    def target_plane(j):
        if j == last:
            return plane
        right_first = jnp.where(j < rights, last - j, j - rights)
        left_first = jnp.where(j < lefts, j, last - j + lefts)
        return jnp.where(rights > lefts, right_first, left_first)

    def fed(j):
        k = target_plane(j)
        return jnp.where(k > plane, plane > 0, plane < last)

    barrier = pltpu.get_barrier_semaphore()
    for d in range(1, inner):
        peer = plane * inner + lax.rem(seat + d, inner)
        pl.semaphore_signal(barrier, inc=1, device_id={"dev": peer}, device_id_type=MESH)
    for d in range(1, outer):
        peer = lax.rem(plane + d, outer) * inner + seat
        pl.semaphore_signal(barrier, inc=1, device_id={"dev": peer}, device_id_type=MESH)
    pl.semaphore_wait(barrier, inner + outer - 2)

    def plane_copy(src, dst, ssem, rsem, index, d, arriving):
        p = lax.rem(seat + d, inner)
        s = lax.rem(seat + inner - d, inner) if arriving else seat
        return pltpu.make_async_remote_copy(
            src_ref=src.at[(*index, p)],
            dst_ref=dst.at[(*index, s)],
            send_sem=ssem.at[(*index, d)],
            recv_sem=rsem.at[(*index, d)],
            device_id={"dev": plane * inner + p},
            device_id_type=MESH,
        )

    def data_copy(j, c, d, arriving):
        return plane_copy(out, got, send, recv, (j, c), d, arriving)

    def meta_copy(j, d, arriving):
        return plane_copy(mout, mgot, msend, mrecv, (j,), d, arriving)

    def line_copy(j, c):
        k = target_plane(j)
        step = jnp.where(k > plane, 1, -1)
        place = jnp.where(k == plane - 1, outer, k)
        return pltpu.make_async_remote_copy(
            src_ref=zout.at[j, c],
            dst_ref=zin.at[place, c],
            send_sem=zsend.at[j, c],
            recv_sem=zrecv.at[place, c],
            device_id={"dev": (plane + step) * inner + seat},
            device_id_type=MESH,
        )

    def line_arrival(place, c):
        side = jnp.where(plane > 0, -1, 1)
        return pltpu.make_async_remote_copy(
            src_ref=zout.at[0, c],
            dst_ref=zin.at[place, c],
            send_sem=zsend.at[0, c],
            recv_sem=zrecv.at[place, c],
            device_id={"dev": (plane + side) * inner + seat},
            device_id_type=MESH,
        )

    def aux_copy(j, arriving):
        k = target_plane(j)
        return pltpu.make_async_remote_copy(
            src_ref=zaux.at[j],
            dst_ref=zin_aux.at[k if arriving else plane],
            send_sem=asend.at[j],
            recv_sem=arecv.at[k if arriving else plane],
            device_id={"dev": k * inner + seat},
            device_id_type=MESH,
        )

    def gather(j):
        slot = target_plane(j) * (inner * cap) + lax.broadcasted_iota(
            jnp.int32, (inner * cap, rows), 0
        )
        pick = (slot == route_ref[0:1, :]).astype(jnp.bfloat16)
        for c in range(chunks):
            columns = slice(c * chunk, (c + 1) * chunk)
            block = jnp.dot(pick, high[:, columns], preferred_element_type=jnp.float32)
            block = block + jnp.dot(pick, low[:, columns], preferred_element_type=jnp.float32)
            out[j, c] = block.reshape(inner, cap, chunk)
            for d in range(1, inner):
                data_copy(j, c, d, False).start()
        if j == 0:
            value = points_ref[...]
            norms = jnp.sum(value * value, axis=1, keepdims=True)
            norms = jnp.broadcast_to(norms, (rows, LANES)).T[0:1, :]
            label = route_ref[1:2, :].astype(jnp.float32).astype(jnp.bfloat16)
            blank = jnp.zeros((4, rows), jnp.bfloat16)
            facts[...] = jnp.concatenate([label] + pieces(norms, 3) + [blank], axis=0)
        told = lax.dot_general(
            facts[...], pick, (((1,), (1,)), ((), ())), preferred_element_type=jnp.float32
        )
        for p in range(inner):
            mine = told[:, p * cap : (p + 1) * cap]
            mout[j, p] = jnp.concatenate([mine] * rep, axis=1)
        for d in range(1, inner):
            meta_copy(j, d, False).start()

    lane = lax.broadcasted_iota(jnp.int32, (8, LANES), 1)
    line = lax.broadcasted_iota(jnp.int32, (8, LANES), 0)
    cluster = lax.broadcasted_iota(jnp.int32, (CL_OWN, LANES), 0).astype(jnp.float32) + 1.0

    def matches(j):
        for d in range(1, inner):
            meta_copy(j, d, True).wait_recv()
        mgot[j, seat] = mout[j, seat]
        weights = []
        for s in range(inner):
            block = mgot[j, s]
            hit[:, s * LANES : (s + 1) * LANES] = (cluster == block[0:1, :]).astype(jnp.bfloat16)
            block = jnp.where(line == 0, 1.0, block)
            weights.append(jnp.where(lane < cap, block, 0.0).astype(jnp.bfloat16))
        aux = lax.dot_general(
            jnp.concatenate(weights, axis=1), hit[...], (((1,), (1,)), ((), ())),
            preferred_element_type=jnp.float32,
        )
        if j < last:
            zaux[j] = aux
            aux_copy(j, False).start()
        else:
            aux_ref[...] = aux

    def reduce(j, c):
        for d in range(1, inner):
            data_copy(j, c, d, True).wait_recv()
        got[j, c, seat] = out[j, c, seat]
        stack = []
        for s in range(inner):
            stack.extend(pieces(got[j, c, s], rep))
        total = jnp.dot(hit[...], jnp.concatenate(stack, axis=0), preferred_element_type=jnp.float32)
        if j == last:
            sums_ref[:, c * chunk : (c + 1) * chunk] = total
        else:
            zout[j, c] = total

    def forward(j, c):
        @pl.when(fed(j))
        def _():
            k = target_plane(j)
            line_arrival(k, c).wait_recv()
            zout[j, c] += zin[k, c]
            line_copy(j, c).start()

    value = points_ref[...]
    top = value.astype(jnp.bfloat16)
    high[...] = top
    low[...] = (value - top.astype(jnp.float32)).astype(jnp.bfloat16)

    gather(0)
    behind = None
    for j in range(outer):
        if j == 0:
            for later in range(1, outer):
                gather(later)
        matches(j)
        for c in range(chunks):
            reduce(j, c)
            if j < last:
                @pl.when(jnp.logical_not(fed(j)))
                def _():
                    line_copy(j, c).start()
            if behind is not None:
                forward(*behind)
            behind = (j, c) if j < last else None

    for j in range(last):
        aux_copy(j, True).wait_recv()
        aux_ref[...] += zin_aux[target_plane(j)]
    for c in range(chunks):
        columns = slice(c * chunk, (c + 1) * chunk)

        @pl.when(plane > 0)
        def _():
            line_arrival(plane, c).wait_recv()
            sums_ref[:, columns] += zin[plane, c]

        @pl.when(plane < last)
        def _():
            line_arrival(outer, c).wait_recv()
            sums_ref[:, columns] += zin[outer, c]

    for j in range(outer):
        for d in range(1, inner):
            meta_copy(j, d, False).wait_send()
            for c in range(chunks):
                data_copy(j, c, d, False).wait_send()
    for j in range(last):
        aux_copy(j, False).wait_send()
        for c in range(chunks):
            line_copy(j, c).wait_send()


def body(points, assignment):
    owners = lax.axis_size("dev")
    rows, width = points.shape
    cap = 2 * rows // owners
    inner = 1
    while 4 * inner * inner <= 2 * owners:
        inner *= 2
    outer = owners // inner
    chunk = width // 3 if width % (3 * LANES) == 0 else width
    chunks = width // chunk

    owner = assignment // CL_OWN
    local_label = assignment % CL_OWN
    matches = (owner[:, None] == jnp.arange(owners, dtype=jnp.int32)[None, :]).astype(jnp.float32)
    earlier = (jnp.arange(rows)[:, None] > jnp.arange(rows)[None, :]).astype(jnp.float32)
    before = jnp.dot(earlier, matches, preferred_element_type=jnp.float32)
    position = jnp.sum(before * matches, axis=1).astype(jnp.int32)
    target = owner * cap + position
    route = jnp.stack([target, local_label + 1])

    f32, b16 = jnp.float32, jnp.bfloat16
    dma = pltpu.SemaphoreType.DMA
    hops = max(outer - 1, 1)
    sums, aux = pl.pallas_call(
        functools.partial(kernel, inner, outer, cap, chunk),
        out_shape=(
            jax.ShapeDtypeStruct((CL_OWN, width), f32),
            jax.ShapeDtypeStruct((8, CL_OWN), f32),
        ),
        in_specs=[pl.BlockSpec(memory_space=pltpu.VMEM)] * 2,
        out_specs=[pl.BlockSpec(memory_space=pltpu.VMEM)] * 2,
        scratch_shapes=[
            pltpu.VMEM((rows, width), b16),
            pltpu.VMEM((rows, width), b16),
            pltpu.VMEM((8, rows), b16),
            pltpu.VMEM((CL_OWN, inner * LANES), b16),
            pltpu.VMEM((outer, chunks, inner, cap, chunk), f32),
            pltpu.VMEM((outer, chunks, inner, cap, chunk), f32),
            pltpu.VMEM((outer, inner, 8, LANES), f32),
            pltpu.VMEM((outer, inner, 8, LANES), f32),
            pltpu.VMEM((hops, chunks, CL_OWN, chunk), f32),
            pltpu.VMEM((outer + 1, chunks, CL_OWN, chunk), f32),
            pltpu.VMEM((hops, 8, CL_OWN), f32),
            pltpu.VMEM((outer, 8, CL_OWN), f32),
            dma((outer, inner)), dma((outer, inner)),
            dma((outer, chunks, inner)), dma((outer, chunks, inner)),
            dma((hops, chunks)), dma((outer + 1, chunks)),
            dma((hops,)), dma((outer,)),
        ],
        compiler_params=pltpu.CompilerParams(
            collective_id=0, has_side_effects=True, vmem_limit_bytes=60 * 1024 * 1024
        ),
    )(points, route)
    counts = aux[0]
    squares = aux[1] + aux[2] + aux[3]
    sums, counts, squares = lax.psum((sums, counts, squares), "grp")
    return finish(sums, counts, squares)


def solution(mesh):
    return jax.shard_map(
        body,
        mesh=mesh,
        in_specs=(P(("grp", "dev"), None), P(("grp", "dev"))),
        out_specs=(P("dev", None), P("dev")),
        check_vma=False,
    )
```

```python
import functools

import jax
import jax.numpy as jnp
from jax import lax
from jax.experimental import pallas as pl
from jax.experimental.pallas import tpu as pltpu
from jax.sharding import PartitionSpec as P

CL_OWN = 256
LANES = 128
MESH = pl.DeviceIdType.MESH


def finish(sums, counts, squares):
    denom = jnp.maximum(counts, 1.0)
    centre = sums / denom[:, None]
    spread = (squares - jnp.sum(sums * sums, axis=1) / denom) / (denom * sums.shape[1])
    return (centre, spread)


def pieces(value, count):
    out = []
    for _ in range(count):
        part = value.astype(jnp.bfloat16)
        out.append(part)
        value = value - part.astype(jnp.float32)
    return out


def kernel(
    inner, outer, cap, chunk,
    points_ref, route_ref, sums_ref, aux_ref,
    high, low, facts, hit, out, got, relay, mout, mgot, zout, zin, zaux, zin_aux,
    msend, mrecv, send, recv, rsend, rrecv, zsend, zrecv, asend, arecv,
):
    me = lax.axis_index("dev")
    plane = me // inner
    seat = lax.rem(me, inner)
    rows, width = points_ref.shape
    chunks = width // chunk
    rep = LANES // cap
    last = outer - 1
    rights, lefts = last - plane, plane

    def target_plane(j):
        if j == last:
            return plane
        right_first = jnp.where(j < rights, last - j, j - rights)
        left_first = jnp.where(j < lefts, j, last - j + lefts)
        return jnp.where(rights > lefts, right_first, left_first)

    def fed(j):
        k = target_plane(j)
        return jnp.where(k > plane, plane > 0, plane < last)

    def across(d):
        other = 0
        for bit in range(3):
            own = lax.rem(seat // 2**bit, 2)
            other = other + (1 - own if d // 2**bit % 2 else own) * 2**bit
        return other

    barrier = pltpu.get_barrier_semaphore()
    for d in range(1, inner):
        peer = plane * inner + across(d)
        pl.semaphore_signal(barrier, inc=1, device_id={"dev": peer}, device_id_type=MESH)
    for d in range(1, outer):
        peer = lax.rem(plane + d, outer) * inner + seat
        pl.semaphore_signal(barrier, inc=1, device_id={"dev": peer}, device_id_type=MESH)
    def plane_copy(src, dst, ssem, rsem, d):
        return pltpu.make_async_remote_copy(
            src_ref=src,
            dst_ref=dst,
            send_sem=ssem,
            recv_sem=rsem,
            device_id={"dev": plane * inner + across(d)},
            device_id_type=MESH,
        )

    def data_copy(j, c, d):
        return plane_copy(
            out.at[j, c, across(d)], got.at[j, c, seat], send.at[j, c, d], recv.at[j, c, d], d
        )

    def relay_out(j, c, d):
        return plane_copy(
            out.at[j, c, across(d)], relay.at[j, c, d - 6], rsend.at[j, c, d - 6],
            rrecv.at[j, c, d - 6], 2,
        )

    def relay_on(j, c, d):
        return plane_copy(
            relay.at[j, c, d - 6], got.at[j, c, across(2)], send.at[j, c, d], recv.at[j, c, d],
            d - 2,
        )

    def data_arrival(j, c, d):
        return plane_copy(
            out.at[j, c, 0], got.at[j, c, across(d)], send.at[j, c, d], recv.at[j, c, d], d
        )

    def meta_copy(j, d, arriving):
        return plane_copy(
            mout.at[j, across(d)], mgot.at[j, across(d) if arriving else seat],
            msend.at[j, d], mrecv.at[j, d], d,
        )

    def line_copy(j, c):
        k = target_plane(j)
        step = jnp.where(k > plane, 1, -1)
        place = jnp.where(k == plane - 1, outer, k)
        return pltpu.make_async_remote_copy(
            src_ref=zout.at[j, c],
            dst_ref=zin.at[place, c],
            send_sem=zsend.at[j, c],
            recv_sem=zrecv.at[place, c],
            device_id={"dev": (plane + step) * inner + seat},
            device_id_type=MESH,
        )

    def line_arrival(place, c):
        side = jnp.where(plane > 0, -1, 1)
        return pltpu.make_async_remote_copy(
            src_ref=zout.at[0, c],
            dst_ref=zin.at[place, c],
            send_sem=zsend.at[0, c],
            recv_sem=zrecv.at[place, c],
            device_id={"dev": (plane + side) * inner + seat},
            device_id_type=MESH,
        )

    def aux_copy(j, arriving):
        k = target_plane(j)
        return pltpu.make_async_remote_copy(
            src_ref=zaux.at[j],
            dst_ref=zin_aux.at[k if arriving else plane],
            send_sem=asend.at[j],
            recv_sem=arecv.at[k if arriving else plane],
            device_id={"dev": k * inner + seat},
            device_id_type=MESH,
        )

    steps = outer * chunks
    ahead = min(2, steps)

    def own_y(t):
        for d in (4, 5):
            data_copy(t // chunks, t % chunks, d).start()

    def pass_on(t):
        for d in (6, 7):
            relay_out(t // chunks, t % chunks, d).wait_recv()
            relay_on(t // chunks, t % chunks, d).start()
        if t + ahead < steps:
            own_y(t + ahead)

    def gather(j):
        slot = target_plane(j) * (inner * cap) + lax.broadcasted_iota(
            jnp.int32, (inner * cap, rows), 0
        )
        pick = (slot == route_ref[0:1, :]).astype(jnp.bfloat16)
        for c in range(chunks):
            columns = slice(c * chunk, (c + 1) * chunk)
            block = jnp.dot(pick, high[:, columns], preferred_element_type=jnp.float32)
            block = block + jnp.dot(pick, low[:, columns], preferred_element_type=jnp.float32)
            out[j, c] = block.reshape(inner, cap, chunk)
            if j == 0 and c == 0:
                pl.semaphore_wait(barrier, inner + outer - 2)
            for d in (6, 7):
                relay_out(j, c, d).start()
            for d in (2, 3, 1):
                data_copy(j, c, d).start()
            if j * chunks + c < ahead:
                own_y(j * chunks + c)
        if j == 0:
            value = points_ref[...]
            norms = jnp.sum(value * value, axis=1, keepdims=True)
            norms = jnp.broadcast_to(norms, (rows, LANES)).T[0:1, :]
            label = route_ref[1:2, :].astype(jnp.float32).astype(jnp.bfloat16)
            blank = jnp.zeros((4, rows), jnp.bfloat16)
            facts[...] = jnp.concatenate([label] + pieces(norms, 3) + [blank], axis=0)
        told = lax.dot_general(
            facts[...], pick, (((1,), (1,)), ((), ())), preferred_element_type=jnp.float32
        )
        for p in range(inner):
            mine = told[:, p * cap : (p + 1) * cap]
            mout[j, p] = jnp.concatenate([mine] * rep, axis=1)
        for d in range(1, inner):
            meta_copy(j, d, False).start()

    lane = lax.broadcasted_iota(jnp.int32, (8, LANES), 1)
    line = lax.broadcasted_iota(jnp.int32, (8, LANES), 0)
    cluster = lax.broadcasted_iota(jnp.int32, (CL_OWN, LANES), 0).astype(jnp.float32) + 1.0

    def matches(j):
        for d in range(1, inner):
            meta_copy(j, d, True).wait_recv()
        mgot[j, seat] = mout[j, seat]
        weights = []
        for s in range(inner):
            block = mgot[j, s]
            hit[:, s * LANES : (s + 1) * LANES] = (cluster == block[0:1, :]).astype(jnp.bfloat16)
            block = jnp.where(line == 0, 1.0, block)
            weights.append(jnp.where(lane < cap, block, 0.0).astype(jnp.bfloat16))
        aux = lax.dot_general(
            jnp.concatenate(weights, axis=1), hit[...], (((1,), (1,)), ((), ())),
            preferred_element_type=jnp.float32,
        )
        if j < last:
            zaux[j] = aux
            aux_copy(j, False).start()
        else:
            aux_ref[...] = aux

    def reduce(j, c):
        for d in range(1, inner):
            data_arrival(j, c, d).wait_recv()
        got[j, c, seat] = out[j, c, seat]
        stack = []
        for s in range(inner):
            stack.extend(pieces(got[j, c, s], rep))
        total = jnp.dot(hit[...], jnp.concatenate(stack, axis=0), preferred_element_type=jnp.float32)
        if j == last:
            sums_ref[:, c * chunk : (c + 1) * chunk] = total
        else:
            zout[j, c] = total

    def forward(j, c):
        @pl.when(fed(j))
        def _():
            k = target_plane(j)
            line_arrival(k, c).wait_recv()
            zout[j, c] += zin[k, c]
            line_copy(j, c).start()

    value = points_ref[...]
    top = value.astype(jnp.bfloat16)
    high[...] = top
    low[...] = (value - top.astype(jnp.float32)).astype(jnp.bfloat16)

    gather(0)
    passed = 0
    for j in range(1, outer):
        gather(j)
        if j < outer - 1 and passed < steps:
            pass_on(passed)
            passed += 1
    behind = None
    for j in range(outer):
        for c in range(chunks):
            while passed < min(j * chunks + c + 2, steps):
                pass_on(passed)
                passed += 1
            if c == 0:
                matches(j)
            reduce(j, c)
            if j < last:
                @pl.when(jnp.logical_not(fed(j)))
                def _():
                    line_copy(j, c).start()
            if behind is not None:
                forward(*behind)
            behind = (j, c) if j < last else None

    for j in range(last):
        aux_copy(j, True).wait_recv()
        aux_ref[...] += zin_aux[target_plane(j)]
    for c in range(chunks):
        columns = slice(c * chunk, (c + 1) * chunk)

        @pl.when(plane > 0)
        def _():
            line_arrival(plane, c).wait_recv()
            sums_ref[:, columns] += zin[plane, c]

        @pl.when(plane < last)
        def _():
            line_arrival(outer, c).wait_recv()
            sums_ref[:, columns] += zin[outer, c]

    for j in range(outer):
        for d in range(1, inner):
            meta_copy(j, d, False).wait_send()
            for c in range(chunks):
                if d < 6:
                    data_copy(j, c, d).wait_send()
                else:
                    relay_out(j, c, d).wait_send()
                    relay_on(j, c, d).wait_send()
    for j in range(last):
        aux_copy(j, False).wait_send()
        for c in range(chunks):
            line_copy(j, c).wait_send()


def body(points, assignment):
    owners = lax.axis_size("dev")
    rows, width = points.shape
    cap = 2 * rows // owners
    inner = 8
    outer = owners // inner
    chunk = width // 3 if width % (3 * LANES) == 0 else width
    chunks = width // chunk

    owner = assignment // CL_OWN
    local_label = assignment % CL_OWN
    matches = (owner[:, None] == jnp.arange(owners, dtype=jnp.int32)[None, :]).astype(jnp.float32)
    earlier = (jnp.arange(rows)[:, None] > jnp.arange(rows)[None, :]).astype(jnp.float32)
    before = jnp.dot(earlier, matches, preferred_element_type=jnp.float32)
    position = jnp.sum(before * matches, axis=1).astype(jnp.int32)
    target = owner * cap + position
    route = jnp.stack([target, local_label + 1])

    f32, b16 = jnp.float32, jnp.bfloat16
    dma = pltpu.SemaphoreType.DMA
    hops = max(outer - 1, 1)
    sums, aux = pl.pallas_call(
        functools.partial(kernel, inner, outer, cap, chunk),
        out_shape=(
            jax.ShapeDtypeStruct((CL_OWN, width), f32),
            jax.ShapeDtypeStruct((8, CL_OWN), f32),
        ),
        in_specs=[pl.BlockSpec(memory_space=pltpu.VMEM)] * 2,
        out_specs=[pl.BlockSpec(memory_space=pltpu.VMEM)] * 2,
        scratch_shapes=[
            pltpu.VMEM((rows, width), b16),
            pltpu.VMEM((rows, width), b16),
            pltpu.VMEM((8, rows), b16),
            pltpu.VMEM((CL_OWN, inner * LANES), b16),
            pltpu.VMEM((outer, chunks, inner, cap, chunk), f32),
            pltpu.VMEM((outer, chunks, inner, cap, chunk), f32),
            pltpu.VMEM((outer, chunks, 2, cap, chunk), f32),
            pltpu.VMEM((outer, inner, 8, LANES), f32),
            pltpu.VMEM((outer, inner, 8, LANES), f32),
            pltpu.VMEM((hops, chunks, CL_OWN, chunk), f32),
            pltpu.VMEM((outer + 1, chunks, CL_OWN, chunk), f32),
            pltpu.VMEM((hops, 8, CL_OWN), f32),
            pltpu.VMEM((outer, 8, CL_OWN), f32),
            dma((outer, inner)), dma((outer, inner)),
            dma((outer, chunks, inner)), dma((outer, chunks, inner)),
            dma((outer, chunks, 2)), dma((outer, chunks, 2)),
            dma((hops, chunks)), dma((outer + 1, chunks)),
            dma((hops,)), dma((outer,)),
        ],
        compiler_params=pltpu.CompilerParams(
            collective_id=0, has_side_effects=True, vmem_limit_bytes=60 * 1024 * 1024
        ),
    )(points, route)
    counts = aux[0]
    squares = aux[1] + aux[2] + aux[3]
    sums, counts, squares = lax.psum((sums, counts, squares), "grp")
    return finish(sums, counts, squares)


def solution(mesh):
    return jax.shard_map(
        body,
        mesh=mesh,
        in_specs=(P(("grp", "dev"), None), P(("grp", "dev"))),
        out_specs=(P("dev", None), P("dev")),
        check_vma=False,
    )
```

```python
import functools

import jax
import jax.numpy as jnp
from jax import lax
from jax.experimental import pallas as pl
from jax.experimental.pallas import tpu as pltpu
from jax.sharding import PartitionSpec as P

CL_OWN = 256
LANES = 128
MESH = pl.DeviceIdType.MESH


def finish(sums, counts, squares):
    denom = jnp.maximum(counts, 1.0)
    centre = sums / denom[:, None]
    spread = (squares - jnp.sum(sums * sums, axis=1) / denom) / (denom * sums.shape[1])
    return (centre, spread)


def pieces(value, count):
    out = []
    for _ in range(count):
        part = value.astype(jnp.bfloat16)
        out.append(part)
        value = value - part.astype(jnp.float32)
    return out


def kernel(
    inner, outer, cap, chunk,
    points_ref, route_ref, sums_ref, aux_ref,
    high, low, facts, hit, hold, cout, xin, yin, mout, mgot, zout, zin, zaux, zin_aux,
    msend, mrecv, csend, crecv, xsend, xrecv, ysend, yrecv, zsend, zrecv, asend, arecv,
):
    me = lax.axis_index("dev")
    plane = me // inner
    seat = lax.rem(me, inner)
    rows, width = points_ref.shape
    chunks = width // chunk
    rep = LANES // cap
    last = outer - 1
    rights, lefts = last - plane, plane

    def target_plane(j):
        if j == last:
            return plane
        right_first = jnp.where(j < rights, last - j, j - rights)
        left_first = jnp.where(j < lefts, j, last - j + lefts)
        return jnp.where(rights > lefts, right_first, left_first)

    def fed(j):
        k = target_plane(j)
        return jnp.where(k > plane, plane > 0, plane < last)

    def across(d):
        other = 0
        for bit in range(3):
            own = lax.rem(seat // 2**bit, 2)
            other = other + (1 - own if d // 2**bit % 2 else own) * 2**bit
        return other

    barrier = pltpu.get_barrier_semaphore()
    for d in range(1, inner):
        peer = plane * inner + across(d)
        pl.semaphore_signal(barrier, inc=1, device_id={"dev": peer}, device_id_type=MESH)
    for d in range(1, outer):
        peer = lax.rem(plane + d, outer) * inner + seat
        pl.semaphore_signal(barrier, inc=1, device_id={"dev": peer}, device_id_type=MESH)
    def plane_copy(src, dst, ssem, rsem, d):
        return pltpu.make_async_remote_copy(
            src_ref=src,
            dst_ref=dst,
            send_sem=ssem,
            recv_sem=rsem,
            device_id={"dev": plane * inner + across(d)},
            device_id_type=MESH,
        )

    core = lax.rem(seat, 2)
    x = lax.rem(seat // 2, 2)
    y = seat // 4

    def core_copy(t):
        j, c = t // chunks, t % chunks
        return plane_copy(
            cout.at[j, c], hold.at[j, c, :, core], csend.at[j, c], crecv.at[j, c], 1
        )

    def core_arrival(t):
        j, c = t // chunks, t % chunks
        return plane_copy(
            cout.at[j, c], hold.at[j, c, :, 1 - core], csend.at[j, c], crecv.at[j, c], 1
        )

    def x_copy(t):
        j, c = t // chunks, t % chunks
        return plane_copy(
            hold.at[j, c, pl.ds((1 - x) * 2, 2)], xin.at[j, c], xsend.at[j, c], xrecv.at[j, c], 2
        )

    def y_copy(t, passed):
        j, c = t // chunks, t % chunks
        source = xin.at[j, c, 1 - y] if passed else hold.at[j, c, x * 2 + 1 - y]
        return plane_copy(
            source, yin.at[j, c, passed], ysend.at[j, c, passed], yrecv.at[j, c, passed], 4
        )

    def meta_copy(d, arriving):
        return plane_copy(
            mout.at[across(d)], mgot.at[across(d) if arriving else seat],
            msend.at[d], mrecv.at[d], d,
        )

    def line_copy(j, c):
        k = target_plane(j)
        step = jnp.where(k > plane, 1, -1)
        place = jnp.where(k == plane - 1, outer, k)
        return pltpu.make_async_remote_copy(
            src_ref=zout.at[j, c],
            dst_ref=zin.at[place, c],
            send_sem=zsend.at[j, c],
            recv_sem=zrecv.at[place, c],
            device_id={"dev": (plane + step) * inner + seat},
            device_id_type=MESH,
        )

    def line_arrival(place, c):
        side = jnp.where(plane > 0, -1, 1)
        return pltpu.make_async_remote_copy(
            src_ref=zout.at[0, c],
            dst_ref=zin.at[place, c],
            send_sem=zsend.at[0, c],
            recv_sem=zrecv.at[place, c],
            device_id={"dev": (plane + side) * inner + seat},
            device_id_type=MESH,
        )

    def aux_copy(j, arriving):
        k = target_plane(j)
        return pltpu.make_async_remote_copy(
            src_ref=zaux.at[j],
            dst_ref=zin_aux.at[k if arriving else plane],
            send_sem=asend.at[j],
            recv_sem=arecv.at[k if arriving else plane],
            device_id={"dev": k * inner + seat},
            device_id_type=MESH,
        )

    steps = outer * chunks
    ahead = 3
    half = inner // 2 * cap

    def picks(j):
        row = lax.broadcasted_iota(jnp.int32, (2 * half, 1), 0)
        slot = target_plane(j) * (2 * half) + row
        slot = slot + jnp.where(row < half, core * half, -core * half)
        return (slot == route_ref[0:1, :]).astype(jnp.bfloat16)

    def gather(t, pick):
        j, c = t // chunks, t % chunks
        columns = slice(c * chunk, (c + 1) * chunk)
        block = jnp.dot(pick, high[:, columns], preferred_element_type=jnp.float32)
        block = block + jnp.dot(pick, low[:, columns], preferred_element_type=jnp.float32)
        hold[j, c, :, core] = block[:half].reshape(inner // 2, cap, chunk)
        cout[j, c] = block[half:].reshape(inner // 2, cap, chunk)
        if t == 0:
            pl.semaphore_wait(barrier, inner + outer - 2)
        core_copy(t).start()

    def launch(t):
        core_arrival(t).wait_recv()
        x_copy(t).start()
        y_copy(t, 0).start()

    def pass_on(t):
        x_copy(t).wait_recv()
        y_copy(t, 1).start()
        if t + ahead < steps:
            launch(t + ahead)

    def tell():
        value = points_ref[...]
        norms = jnp.sum(value * value, axis=1, keepdims=True)
        norms = jnp.broadcast_to(norms, (rows, LANES)).T[0:1, :]
        label = route_ref[1:2, :].astype(jnp.float32).astype(jnp.bfloat16)
        blank = jnp.zeros((4, rows), jnp.bfloat16)
        facts[...] = jnp.concatenate([label] + pieces(norms, 3) + [blank], axis=0)

    def tell_slots(j, pick):
        told = lax.dot_general(
            facts[...], pick, (((1,), (1,)), ((), ())), preferred_element_type=jnp.float32
        )
        for q in range(inner):
            p = q % 2 * 4 + q // 2 % 2 * 2 + (core if q < inner // 2 else 1 - core)
            mine = told[:, q * cap : (q + 1) * cap]
            mout[p, j] = jnp.concatenate([mine] * rep, axis=1)

    lane = lax.broadcasted_iota(jnp.int32, (8, LANES), 1)
    line = lax.broadcasted_iota(jnp.int32, (8, LANES), 0)
    cluster = lax.broadcasted_iota(jnp.int32, (CL_OWN, LANES), 0).astype(jnp.float32) + 1.0

    def matches(j):
        if j == 0:
            for d in range(1, inner):
                meta_copy(d, True).wait_recv()
            mgot[seat] = mout[seat]
        weights = []
        for s in range(inner):
            block = mgot[across(s // 2 * 2) - core + s % 2, j]
            hit[:, s * LANES : (s + 1) * LANES] = (cluster == block[0:1, :]).astype(jnp.bfloat16)
            block = jnp.where(line == 0, 1.0, block)
            weights.append(jnp.where(lane < cap, block, 0.0).astype(jnp.bfloat16))
        aux = lax.dot_general(
            jnp.concatenate(weights, axis=1), hit[...], (((1,), (1,)), ((), ())),
            preferred_element_type=jnp.float32,
        )
        if j < last:
            zaux[j] = aux
            aux_copy(j, False).start()
        else:
            aux_ref[...] = aux

    def reduce(j, c):
        t = j * chunks + c
        y_copy(t, 0).wait_recv()
        y_copy(t, 1).wait_recv()
        stack = []
        for ref in (hold.at[j, c, x * 2 + y], xin.at[j, c, y], yin.at[j, c, 0], yin.at[j, c, 1]):
            for s in range(2):
                stack.extend(pieces(ref[s], rep))
        total = jnp.dot(hit[...], jnp.concatenate(stack, axis=0), preferred_element_type=jnp.float32)
        if j == last:
            sums_ref[:, c * chunk : (c + 1) * chunk] = total
        else:
            zout[j, c] = total

    def forward(j, c):
        @pl.when(fed(j))
        def _():
            k = target_plane(j)
            line_arrival(k, c).wait_recv()
            zout[j, c] += zin[k, c]
            line_copy(j, c).start()

    value = points_ref[...]
    top = value.astype(jnp.bfloat16)
    high[...] = top
    low[...] = (value - top.astype(jnp.float32)).astype(jnp.bfloat16)

    pick = picks(0)
    gather(0, pick)
    tell()
    launch(0)
    for j in range(outer):
        tell_slots(j, picks(j))
    for d in range(1, inner):
        meta_copy(d, False).start()
    for t in range(1, chunks):
        gather(t, pick)
    for t in range(1, ahead):
        if t < chunks:
            launch(t)
    passed = 0
    for j in range(1, outer):
        pick = picks(j)
        for c in range(chunks):
            gather(j * chunks + c, pick)
        if j == 1:
            for t in range(chunks, ahead):
                launch(t)
        if j < outer - 1:
            pass_on(passed)
            passed += 1
    behind = None
    for j in range(outer):
        for c in range(chunks):
            while passed < min(j * chunks + c + 2, steps):
                pass_on(passed)
                passed += 1
            if c == 0:
                matches(j)
            reduce(j, c)
            if j < last:
                @pl.when(jnp.logical_not(fed(j)))
                def _():
                    line_copy(j, c).start()
            if behind is not None:
                forward(*behind)
            behind = (j, c) if j < last else None

    for j in range(last):
        aux_copy(j, True).wait_recv()
        aux_ref[...] += zin_aux[target_plane(j)]
    for c in range(chunks):
        columns = slice(c * chunk, (c + 1) * chunk)

        @pl.when(plane > 0)
        def _():
            line_arrival(plane, c).wait_recv()
            sums_ref[:, columns] += zin[plane, c]

        @pl.when(plane < last)
        def _():
            line_arrival(outer, c).wait_recv()
            sums_ref[:, columns] += zin[outer, c]

    for d in range(1, inner):
        meta_copy(d, False).wait_send()
    for t in range(steps):
        core_copy(t).wait_send()
        x_copy(t).wait_send()
        y_copy(t, 0).wait_send()
        y_copy(t, 1).wait_send()
    for j in range(last):
        aux_copy(j, False).wait_send()
        for c in range(chunks):
            line_copy(j, c).wait_send()


def body(points, assignment):
    owners = lax.axis_size("dev")
    rows, width = points.shape
    cap = 2 * rows // owners
    inner = 8
    outer = owners // inner
    chunk = width // 3 if width % (3 * LANES) == 0 else width
    chunks = width // chunk

    owner = assignment // CL_OWN
    local_label = assignment % CL_OWN
    matches = (owner[:, None] == jnp.arange(owners, dtype=jnp.int32)[None, :]).astype(jnp.float32)
    earlier = (jnp.arange(rows)[:, None] > jnp.arange(rows)[None, :]).astype(jnp.float32)
    before = jnp.dot(earlier, matches, preferred_element_type=jnp.float32)
    position = jnp.sum(before * matches, axis=1).astype(jnp.int32)
    seat = owner % inner
    place = owner - seat + seat % 2 * 4 + seat // 2 % 2 * 2 + seat // 4
    target = place * cap + position
    route = jnp.stack([target, local_label + 1])

    f32, b16 = jnp.float32, jnp.bfloat16
    dma = pltpu.SemaphoreType.DMA
    hops = max(outer - 1, 1)
    sums, aux = pl.pallas_call(
        functools.partial(kernel, inner, outer, cap, chunk),
        out_shape=(
            jax.ShapeDtypeStruct((CL_OWN, width), f32),
            jax.ShapeDtypeStruct((8, CL_OWN), f32),
        ),
        in_specs=[pl.BlockSpec(memory_space=pltpu.VMEM)] * 2,
        out_specs=[pl.BlockSpec(memory_space=pltpu.VMEM)] * 2,
        scratch_shapes=[
            pltpu.VMEM((rows, width), b16),
            pltpu.VMEM((rows, width), b16),
            pltpu.VMEM((8, rows), b16),
            pltpu.VMEM((CL_OWN, inner * LANES), b16),
            pltpu.VMEM((outer, chunks, inner // 2, 2, cap, chunk), f32),
            pltpu.VMEM((outer, chunks, inner // 2, cap, chunk), f32),
            pltpu.VMEM((outer, chunks, 2, 2, cap, chunk), f32),
            pltpu.VMEM((outer, chunks, 2, 2, cap, chunk), f32),
            pltpu.VMEM((inner, outer, 8, LANES), f32),
            pltpu.VMEM((inner, outer, 8, LANES), f32),
            pltpu.VMEM((hops, chunks, CL_OWN, chunk), f32),
            pltpu.VMEM((outer + 1, chunks, CL_OWN, chunk), f32),
            pltpu.VMEM((hops, 8, CL_OWN), f32),
            pltpu.VMEM((outer, 8, CL_OWN), f32),
            dma((inner,)), dma((inner,)),
            dma((outer, chunks)), dma((outer, chunks)),
            dma((outer, chunks)), dma((outer, chunks)),
            dma((outer, chunks, 2)), dma((outer, chunks, 2)),
            dma((hops, chunks)), dma((outer + 1, chunks)),
            dma((hops,)), dma((outer,)),
        ],
        compiler_params=pltpu.CompilerParams(
            collective_id=0, has_side_effects=True, vmem_limit_bytes=60 * 1024 * 1024
        ),
    )(points, route)
    counts = aux[0]
    squares = aux[1] + aux[2] + aux[3]
    sums, counts, squares = lax.psum((sums, counts, squares), "grp")
    return finish(sums, counts, squares)


def solution(mesh):
    return jax.shard_map(
        body,
        mesh=mesh,
        in_specs=(P(("grp", "dev"), None), P(("grp", "dev"))),
        out_specs=(P("dev", None), P("dev")),
        check_vma=False,
    )
```

```python
import functools

import jax
import jax.numpy as jnp
from jax import lax
from jax.experimental import pallas as pl
from jax.experimental.pallas import tpu as pltpu
from jax.sharding import PartitionSpec as P

CL_OWN = 256
LANES = 128
MESH = pl.DeviceIdType.MESH


def finish(sums, counts, squares):
    denom = jnp.maximum(counts, 1.0)
    centre = sums / denom[:, None]
    spread = (squares - jnp.sum(sums * sums, axis=1) / denom) / (denom * sums.shape[1])
    return (centre, spread)


def pieces(value, count):
    out = []
    for _ in range(count):
        part = value.astype(jnp.bfloat16)
        out.append(part)
        value = value - part.astype(jnp.float32)
    return out


def kernel(
    inner, outer, cap, chunk,
    points_ref, route_ref, sums_ref, aux_ref,
    high, low, facts, hit, hold, cout, xin, yin, mout, mgot, zout, zin, zaux, zin_aux,
    msend, mrecv, csend, crecv, xsend, xrecv, ysend, yrecv, zsend, zrecv, asend, arecv,
):
    me = lax.axis_index("dev")
    plane = me // inner
    seat = lax.rem(me, inner)
    rows, width = points_ref.shape
    chunks = width // chunk
    rep = LANES // cap
    last = outer - 1
    rights, lefts = last - plane, plane

    def target_plane(j):
        if j == last:
            return plane
        right_first = jnp.where(j < rights, last - j, j - rights)
        left_first = jnp.where(j < lefts, j, last - j + lefts)
        return jnp.where(rights > lefts, right_first, left_first)

    def fed(j):
        k = target_plane(j)
        return jnp.where(k > plane, plane > 0, plane < last)

    def across(d):
        other = 0
        for bit in range(3):
            own = lax.rem(seat // 2**bit, 2)
            other = other + (1 - own if d // 2**bit % 2 else own) * 2**bit
        return other

    barrier = pltpu.get_barrier_semaphore()
    for d in range(1, inner):
        peer = plane * inner + across(d)
        pl.semaphore_signal(barrier, inc=1, device_id={"dev": peer}, device_id_type=MESH)
    for d in range(1, outer):
        peer = lax.rem(plane + d, outer) * inner + seat
        pl.semaphore_signal(barrier, inc=1, device_id={"dev": peer}, device_id_type=MESH)
    def plane_copy(src, dst, ssem, rsem, d):
        return pltpu.make_async_remote_copy(
            src_ref=src,
            dst_ref=dst,
            send_sem=ssem,
            recv_sem=rsem,
            device_id={"dev": plane * inner + across(d)},
            device_id_type=MESH,
        )

    core = lax.rem(seat, 2)
    x = lax.rem(seat // 2, 2)
    y = seat // 4

    def core_copy(t):
        j, c = t // chunks, t % chunks
        return plane_copy(
            cout.at[j, c], hold.at[j, c, :, core], csend.at[j, c], crecv.at[j, c], 1
        )

    def core_arrival(t):
        j, c = t // chunks, t % chunks
        return plane_copy(
            cout.at[j, c], hold.at[j, c, :, 1 - core], csend.at[j, c], crecv.at[j, c], 1
        )

    def x_copy(t):
        j, c = t // chunks, t % chunks
        return plane_copy(
            hold.at[j, c, pl.ds((1 - x) * 2, 2)], xin.at[j, c], xsend.at[j, c], xrecv.at[j, c], 2
        )

    def y_copy(t, passed):
        j, c = t // chunks, t % chunks
        source = xin.at[j, c, 1 - y] if passed else hold.at[j, c, x * 2 + 1 - y]
        return plane_copy(
            source, yin.at[j, c, passed], ysend.at[j, c, passed], yrecv.at[j, c, passed], 4
        )

    def meta_copy(d, arriving):
        return plane_copy(
            mout.at[across(d)], mgot.at[across(d) if arriving else seat],
            msend.at[d], mrecv.at[d], d,
        )

    def line_copy(j, c):
        k = target_plane(j)
        step = jnp.where(k > plane, 1, -1)
        place = jnp.where(k == plane - 1, outer, k)
        return pltpu.make_async_remote_copy(
            src_ref=zout.at[j, c],
            dst_ref=zin.at[place, c],
            send_sem=zsend.at[j, c],
            recv_sem=zrecv.at[place, c],
            device_id={"dev": (plane + step) * inner + seat},
            device_id_type=MESH,
        )

    def line_arrival(place, c):
        side = jnp.where(plane > 0, -1, 1)
        return pltpu.make_async_remote_copy(
            src_ref=zout.at[0, c],
            dst_ref=zin.at[place, c],
            send_sem=zsend.at[0, c],
            recv_sem=zrecv.at[place, c],
            device_id={"dev": (plane + side) * inner + seat},
            device_id_type=MESH,
        )

    def aux_copy(j, arriving):
        k = target_plane(j)
        return pltpu.make_async_remote_copy(
            src_ref=zaux.at[j],
            dst_ref=zin_aux.at[k if arriving else plane],
            send_sem=asend.at[j],
            recv_sem=arecv.at[k if arriving else plane],
            device_id={"dev": k * inner + seat},
            device_id_type=MESH,
        )

    steps = outer * chunks
    ahead = 2
    half = inner // 2 * cap

    def picks(j):
        row = lax.broadcasted_iota(jnp.int32, (2 * half, 1), 0)
        slot = target_plane(j) * (2 * half) + row
        slot = slot + jnp.where(row < half, core * half, -core * half)
        return (slot == route_ref[0:1, :]).astype(jnp.bfloat16)

    def gather(t, pick):
        j, c = t // chunks, t % chunks
        columns = slice(c * chunk, (c + 1) * chunk)
        block = jnp.dot(pick, high[:, columns], preferred_element_type=jnp.float32)
        block = block + jnp.dot(pick, low[:, columns], preferred_element_type=jnp.float32)
        hold[j, c, :, core] = block[:half].reshape(inner // 2, cap, chunk)
        cout[j, c] = block[half:].reshape(inner // 2, cap, chunk)
        if t == 0:
            pl.semaphore_wait(barrier, inner + outer - 2)
        core_copy(t).start()

    def launch(t):
        core_arrival(t).wait_recv()
        x_copy(t).start()
        y_copy(t, 0).start()

    def pass_on(t):
        x_copy(t).wait_recv()
        y_copy(t, 1).start()
        if t + ahead < steps:
            launch(t + ahead)

    def tell():
        value = points_ref[...]
        norms = jnp.sum(value * value, axis=1, keepdims=True)
        norms = jnp.broadcast_to(norms, (rows, LANES)).T[0:1, :]
        label = route_ref[1:2, :].astype(jnp.float32).astype(jnp.bfloat16)
        blank = jnp.zeros((4, rows), jnp.bfloat16)
        facts[...] = jnp.concatenate([label] + pieces(norms, 3) + [blank], axis=0)

    def tell_slots(j, pick):
        told = lax.dot_general(
            facts[...], pick, (((1,), (1,)), ((), ())), preferred_element_type=jnp.float32
        )
        for q in range(inner):
            p = q % 2 * 4 + q // 2 % 2 * 2 + (core if q < inner // 2 else 1 - core)
            mine = told[:, q * cap : (q + 1) * cap]
            mout[p, j] = jnp.concatenate([mine] * rep, axis=1)

    lane = lax.broadcasted_iota(jnp.int32, (8, LANES), 1)
    line = lax.broadcasted_iota(jnp.int32, (8, LANES), 0)
    cluster = lax.broadcasted_iota(jnp.int32, (CL_OWN, LANES), 0).astype(jnp.float32) + 1.0

    def matches(j):
        if j == 0:
            for d in range(1, inner):
                meta_copy(d, True).wait_recv()
            mgot[seat] = mout[seat]
        weights = []
        for s in range(inner):
            block = mgot[across(s // 2 * 2) - core + s % 2, j]
            hit[:, s * LANES : (s + 1) * LANES] = (cluster == block[0:1, :]).astype(jnp.bfloat16)
            block = jnp.where(line == 0, 1.0, block)
            weights.append(jnp.where(lane < cap, block, 0.0).astype(jnp.bfloat16))
        aux = lax.dot_general(
            jnp.concatenate(weights, axis=1), hit[...], (((1,), (1,)), ((), ())),
            preferred_element_type=jnp.float32,
        )
        if j < last:
            zaux[j] = aux
            aux_copy(j, False).start()
        else:
            aux_ref[...] = aux

    def reduce(j, c):
        t = j * chunks + c
        y_copy(t, 0).wait_recv()
        y_copy(t, 1).wait_recv()
        stack = []
        for ref in (hold.at[j, c, x * 2 + y], xin.at[j, c, y], yin.at[j, c, 0], yin.at[j, c, 1]):
            for s in range(2):
                stack.extend(pieces(ref[s], rep))
        total = jnp.dot(hit[...], jnp.concatenate(stack, axis=0), preferred_element_type=jnp.float32)
        if j == last:
            sums_ref[:, c * chunk : (c + 1) * chunk] = total
        else:
            zout[j, c] = total

    def forward(j, c):
        @pl.when(fed(j))
        def _():
            k = target_plane(j)
            line_arrival(k, c).wait_recv()
            zout[j, c] += zin[k, c]
            line_copy(j, c).start()

    value = points_ref[...]
    top = value.astype(jnp.bfloat16)
    high[...] = top
    low[...] = (value - top.astype(jnp.float32)).astype(jnp.bfloat16)

    pick = picks(0)
    gather(0, pick)
    tell()
    launch(0)
    for j in range(outer):
        tell_slots(j, picks(j))
    for d in range(1, inner):
        meta_copy(d, False).start()
    for t in range(1, chunks):
        gather(t, pick)
    for t in range(1, ahead):
        if t < chunks:
            launch(t)
    passed = 0
    for j in range(1, outer):
        pick = picks(j)
        for c in range(chunks):
            gather(j * chunks + c, pick)
        if j == 1:
            for t in range(chunks, ahead):
                launch(t)
        if j < outer - 1:
            pass_on(passed)
            passed += 1
    behind = None
    for j in range(outer):
        for c in range(chunks):
            while passed < min(j * chunks + c + 2, steps):
                pass_on(passed)
                passed += 1
            if c == 0:
                matches(j)
            reduce(j, c)
            if j < last:
                @pl.when(jnp.logical_not(fed(j)))
                def _():
                    line_copy(j, c).start()
            if behind is not None:
                forward(*behind)
            behind = (j, c) if j < last else None

    for j in range(last):
        aux_copy(j, True).wait_recv()
        aux_ref[...] += zin_aux[target_plane(j)]
    for c in range(chunks):
        columns = slice(c * chunk, (c + 1) * chunk)

        @pl.when(plane > 0)
        def _():
            line_arrival(plane, c).wait_recv()
            sums_ref[:, columns] += zin[plane, c]

        @pl.when(plane < last)
        def _():
            line_arrival(outer, c).wait_recv()
            sums_ref[:, columns] += zin[outer, c]

    for d in range(1, inner):
        meta_copy(d, False).wait_send()
    for t in range(steps):
        core_copy(t).wait_send()
        x_copy(t).wait_send()
        y_copy(t, 0).wait_send()
        y_copy(t, 1).wait_send()
    for j in range(last):
        aux_copy(j, False).wait_send()
        for c in range(chunks):
            line_copy(j, c).wait_send()


def body(points, assignment):
    owners = lax.axis_size("dev")
    rows, width = points.shape
    cap = 2 * rows // owners
    inner = 8
    outer = owners // inner
    chunk = width // 3 if width % (3 * LANES) == 0 else width
    chunks = width // chunk

    owner = assignment // CL_OWN
    local_label = assignment % CL_OWN
    matches = (owner[:, None] == jnp.arange(owners, dtype=jnp.int32)[None, :]).astype(jnp.float32)
    earlier = (jnp.arange(rows)[:, None] > jnp.arange(rows)[None, :]).astype(jnp.float32)
    before = jnp.dot(earlier, matches, preferred_element_type=jnp.float32)
    position = jnp.sum(before * matches, axis=1).astype(jnp.int32)
    seat = owner % inner
    place = owner - seat + seat % 2 * 4 + seat // 2 % 2 * 2 + seat // 4
    target = place * cap + position
    route = jnp.stack([target, local_label + 1])

    f32, b16 = jnp.float32, jnp.bfloat16
    dma = pltpu.SemaphoreType.DMA
    hops = max(outer - 1, 1)
    sums, aux = pl.pallas_call(
        functools.partial(kernel, inner, outer, cap, chunk),
        out_shape=(
            jax.ShapeDtypeStruct((CL_OWN, width), f32),
            jax.ShapeDtypeStruct((8, CL_OWN), f32),
        ),
        in_specs=[pl.BlockSpec(memory_space=pltpu.VMEM)] * 2,
        out_specs=[pl.BlockSpec(memory_space=pltpu.VMEM)] * 2,
        scratch_shapes=[
            pltpu.VMEM((rows, width), b16),
            pltpu.VMEM((rows, width), b16),
            pltpu.VMEM((8, rows), b16),
            pltpu.VMEM((CL_OWN, inner * LANES), b16),
            pltpu.VMEM((outer, chunks, inner // 2, 2, cap, chunk), f32),
            pltpu.VMEM((outer, chunks, inner // 2, cap, chunk), f32),
            pltpu.VMEM((outer, chunks, 2, 2, cap, chunk), f32),
            pltpu.VMEM((outer, chunks, 2, 2, cap, chunk), f32),
            pltpu.VMEM((inner, outer, 8, LANES), f32),
            pltpu.VMEM((inner, outer, 8, LANES), f32),
            pltpu.VMEM((hops, chunks, CL_OWN, chunk), f32),
            pltpu.VMEM((outer + 1, chunks, CL_OWN, chunk), f32),
            pltpu.VMEM((hops, 8, CL_OWN), f32),
            pltpu.VMEM((outer, 8, CL_OWN), f32),
            dma((inner,)), dma((inner,)),
            dma((outer, chunks)), dma((outer, chunks)),
            dma((outer, chunks)), dma((outer, chunks)),
            dma((outer, chunks, 2)), dma((outer, chunks, 2)),
            dma((hops, chunks)), dma((outer + 1, chunks)),
            dma((hops,)), dma((outer,)),
        ],
        compiler_params=pltpu.CompilerParams(
            collective_id=0, has_side_effects=True, vmem_limit_bytes=60 * 1024 * 1024
        ),
    )(points, route)
    counts = aux[0]
    squares = aux[1] + aux[2] + aux[3]
    sums, counts, squares = lax.psum((sums, counts, squares), "grp")
    return finish(sums, counts, squares)


def solution(mesh):
    return jax.shard_map(
        body,
        mesh=mesh,
        in_specs=(P(("grp", "dev"), None), P(("grp", "dev"))),
        out_specs=(P("dev", None), P("dev")),
        check_vma=False,
    )
```
